256 devices in a mesh: pair: 4 (over z_lo, core), dp: 64 (over z_hi, x, y).
Axes of the slice: x: 4, y: 4, z: 8 (z_hi: 4, z_lo: 2; z = z_hi * 2 + z_lo), core: 2. Of those that a mesh axis runs over, the one named last changes fastest.
Arguments:
- master: float32 [4, 1048576], P('pair', 'dp'), may hold values from -6 to 6
- moment1: float32 [4, 1048576], P('pair', 'dp'), may hold values from -4 to 4
- moment2: float32 [4, 1048576], P('pair', 'dp'), may hold values from 0.05 to 2
- local_grad: bfloat16 [4, 64, 1048576], P('pair', 'dp'), may hold values from -16 to 16
- partner: int32 [64, 4], P('dp'), may hold values from 0 to 3, as said below
Outputs:
- new_master: float32 [4, 64, 2, 16384], P('pair', 'dp')
- new_moment1: float32 [4, 64, 2, 16384], P('pair', 'dp')
- new_moment2: float32 [4, 64, 2, 16384], P('pair', 'dp')
The draws below stay inside these ranges and needn't reach their ends.
Inputs may be any that keep to these rules, and one draw needn't show every extreme that they name: partner[d, partner[d, i]] == i and partner[d, i] != i for every d and i: each row a perfect matching of the 4 pair indices.
All inputs are finite; a program needn't handle non-finite values.
Results may differ from the reference program's by a relative error of at most 0.0003.
Values sent between devices are 32-bit elements; how exact they have to be, the bound alone decides.
No kernel may reach another device: no remote copies, remote signals or barrier semaphores. Data moves between devices by JAX's collectives and lax.ppermute only.
A program may use at most 64 MiB of HBM per device.

```python
import math
import jax
import jax.numpy as jnp
from jax import lax

SH = 16384
NSH = 1048576
N_PAIR = 4
N_DP = 64


def draw_partner(key, part):
    xor_masks = jax.random.randint(key, (N_DP, 1), 1, 4, dtype=jnp.int32)
    return jnp.bitwise_xor(jnp.arange(N_PAIR, dtype=jnp.int32)[None, :], xor_masks)


def with_spikes(entries, own_key, source, target, shards_of, factor):
    owner, partner = [(jnp.arange(entries.shape[dim]) // (entries.shape[dim] // shards_of)).reshape([-1 if axis == dim else 1 for axis in range(entries.ndim)]) for dim in (source, target)]
    chosen = jax.random.permutation(own_key, shards_of)[partner]
    strong = (owner == chosen) | (owner == (partner + shards_of // 2) % shards_of)
    return jnp.where(strong, factor * entries, entries)


def shard_levels(rng, dims, cuts, least, largest):
    def one(axis_at, shards_of):
        draws = jax.random.uniform(jax.random.fold_in(jax.random.fold_in(rng, 6), axis_at), (shards_of,), jnp.float32, least / len(cuts), largest / len(cuts))
        return jnp.repeat(jnp.exp(draws), dims[axis_at] // shards_of).reshape((-1,) + (1,) * (len(dims) - axis_at - 1))

    loudness = one(*cuts[0])
    for cut in cuts[1:]:
        loudness = loudness * one(*cut)
    return loudness


def scatter_about(rng, dims, scale, reach, split=(), kind=jnp.bfloat16):
    result = jax.random.normal(rng, dims, jnp.float32) * scale
    if len(split) > 0:
        result = shard_levels(rng, dims, split, -0.22, 0.18) * result
    return jnp.clip(result, min=-reach, max=reach).astype(kind)


def noise_with(stream_key, shape, deviation, most, shards, heavy, held_as=jnp.bfloat16):
    entries = deviation * jax.random.normal(stream_key, shape, jnp.float32)
    if shards:
        entries = entries * shard_levels(stream_key, shape, shards, -0.22, 0.18)
    return jnp.clip(with_spikes(entries, jax.random.fold_in(stream_key, 3), *heavy), -most, most).astype(held_as)


def setup_inputs(seed: int = 0) -> dict:
    streams_of = jax.random.split(jax.random.key(seed), 6)
    master = scatter_about(streams_of[0], (N_PAIR, NSH), 1.0, 6.0, ((0, 4), (1, 64)), jnp.float32)
    moment1 = scatter_about(streams_of[1], (N_PAIR, NSH), 0.5, 4.0, ((0, 4), (1, 64)), jnp.float32)
    moment2 = jnp.clip(jnp.exp(math.log(2.0) - 3.6888794 * jax.random.uniform(streams_of[2], (N_PAIR, NSH), jnp.float32) ** shard_levels(streams_of[2], (N_PAIR, NSH), ((0, 4), (1, 64)), -0.2, 0.2)), 0.05, 2.0)
    local_grad = noise_with(streams_of[3], (N_PAIR, N_DP, NSH), 1.0, 16.0, ((0, 4), (1, 64)), (1, 2, 64, 4.0))
    partner = draw_partner(jax.random.fold_in(streams_of[5], 71), 0)
    return dict(master=master, moment1=moment1, moment2=moment2, local_grad=local_grad, partner=partner)


beta_one = 0.9
beta_two = 0.95
bias_one = 1.0 - 0.9 ** 10
bias_two = 1.0 - 0.95 ** 10
rate = 0.001
decay = 0.1
eps_value = 1e-08

def adamw_update(weights, first, second, grads, scale):
    scaled = scale * grads
    first_new = beta_one * first + (1.0 - beta_one) * scaled
    second_new = beta_two * second + (1.0 - beta_two) * scaled * scaled
    change = first_new / bias_one / (jnp.sqrt(second_new / bias_two) + eps_value) + decay * weights
    return (weights - rate * change, first_new, second_new)

def reference(master, moment1, moment2, local_grad, partner):
    n_pair = master.shape[0]
    columns = master.shape[1]

    def add_block(index, running):
        return running + lax.dynamic_index_in_dim(local_grad, index, 1, keepdims=False).astype(jnp.float32)
    total = lax.fori_loop(0, N_DP, add_block, jnp.zeros((n_pair, columns), jnp.float32))
    norm2 = jnp.sum(total * total)
    scale = 1.0 / jnp.maximum(jnp.sqrt(norm2 / (n_pair * columns)), 1.0)
    weights, first, second = adamw_update(master, moment1, moment2, total, scale)
    owners = jnp.arange(n_pair, dtype=jnp.int32)
    mates = jnp.transpose(partner).astype(jnp.int32)
    survive = owners[:, None] < mates

    def arrange(values):
        blocks = values.reshape(n_pair, N_DP, SH)
        other = jnp.take_along_axis(blocks, mates[:, :, None], axis=0)
        paired = jnp.stack([blocks, other], axis=2)
        return jnp.where(survive[:, :, None, None], paired, 0.0)
    return (arrange(weights), arrange(first), arrange(second))
```

```python
import jax
import jax.numpy as jnp
from jax import lax
from jax.experimental import pallas as pl
from jax.experimental.pallas import tpu as pltpu
from jax.sharding import Mesh
from jax.sharding import PartitionSpec as P

beta_one = 0.9
beta_two = 0.95
bias_one = 1.0 - 0.9**10
bias_two = 1.0 - 0.95**10
rate = 0.001
decay = 0.1
eps_value = 1e-08


F32 = jnp.float32
LANES = 128


def shifted(value, axis, by):
    n = lax.axis_size(axis)
    return lax.ppermute(value, axis, [(i, (i + by) % n) for i in range(n)])


def crossed(value, axis, mask):
    n = lax.axis_size(axis)
    return lax.ppermute(value, axis, [(i, i ^ mask) for i in range(n)])


def widen(local_grad, place, groups, shard):
    rows = shard // LANES
    flat = [(g, k, o) for g, group in enumerate(groups) for k, o in enumerate(group)]

    def body(place_ref, grad_ref, *refs):
        outs = refs[: len(groups)]
        held, sems = refs[len(groups) :]
        copies = []
        for n, (_, _, (dz, dx, dy)) in enumerate(flat):
            z = (place_ref[0] + dz) % 4
            x = (place_ref[1] + dx) % 4
            y = (place_ref[2] + dy) % 4
            at = pl.multiple_of(((z * 4 + x) * 4 + y) * shard, shard)
            copies.append(pltpu.make_async_copy(grad_ref.at[0, :, pl.ds(at, shard)], held.at[n], sems.at[n]))
        for copy in copies:
            copy.start()
        for n, (g, k, _) in enumerate(flat):
            copies[n].wait()
            outs[g][pl.ds(k * rows, rows), :] = held[n].astype(F32).reshape(rows, LANES)

    return pl.pallas_call(
        body,
        out_shape=[jax.ShapeDtypeStruct((len(group) * rows, LANES), F32) for group in groups],
        in_specs=[pl.BlockSpec(memory_space=pltpu.SMEM), pl.BlockSpec(memory_space=pl.ANY)],
        out_specs=[pl.BlockSpec(memory_space=pltpu.VMEM) for _ in groups],
        scratch_shapes=[pltpu.VMEM((len(flat), 1, shard), jnp.bfloat16), pltpu.SemaphoreType.DMA((len(flat),))],
        cost_estimate=pl.CostEstimate(flops=len(flat) * shard, bytes_accessed=len(flat) * shard * 8, transcendentals=0),
    )(place, local_grad)


def adamw_update(weights, first, second, grads, scale):
    scaled = scale * grads
    first_new = beta_one * first + (1.0 - beta_one) * scaled
    second_new = beta_two * second + (1.0 - beta_two) * scaled * scaled
    change = first_new / bias_one / (jnp.sqrt(second_new / bias_two) + eps_value) + decay * weights
    return (weights - rate * change, first_new, second_new)


def on_device(master, moment1, moment2, local_grad, partner):
    mine = lax.axis_index("pair")
    mate = partner[0, mine]
    mask = mine ^ mate
    survive = mine < mate
    shard = master.shape[1]
    rows = shard // LANES
    count = 4 * 64 * shard
    place = jnp.stack([lax.axis_index("z"), lax.axis_index("x"), lax.axis_index("y")]).astype(jnp.int32)
    four = range(4)

    def by_x(j, kx):
        return [(j, kx, ky) for ky in four]

    def by_y(j, ky):
        return [(j, kx, ky) for kx in four]

    f0, f1, f2, f3 = widen(local_grad, place, [by_x(0, 2), by_x(1, 2), by_y(2, 2), by_y(3, 2)], shard)
    n0, n1, n2, n3 = widen(local_grad, place, [by_x(0, 3), by_x(1, 1), by_y(2, 3), by_y(3, 1)], shard)
    t0, t1, t2, t3, k0, k1, k2, k3 = widen(
        local_grad,
        place,
        [by_x(0, 1), by_x(1, 3), by_y(2, 1), by_y(3, 3), by_x(0, 0), by_x(1, 0), by_y(2, 0), by_y(3, 0)],
        shard,
    )
    f0, f1, f2, f3 = shifted(f0, "x", 1), shifted(f1, "x", -1), shifted(f2, "y", 1), shifted(f3, "y", -1)
    n0, n1, n2, n3 = shifted(n0, "x", -1), shifted(n1, "x", 1), shifted(n2, "y", -1), shifted(n3, "y", 1)
    t0, t1, t2, t3 = (
        shifted(t0 + f0, "x", 1),
        shifted(t1 + f1, "x", -1),
        shifted(t2 + f2, "y", 1),
        shifted(t3 + f3, "y", -1),
    )
    a = [(k + n + t).reshape(4, rows, LANES) for k, n, t in zip((k0, k1, k2, k3), (n0, n1, n2, n3), (t0, t1, t2, t3))]
    ax = [jnp.stack([a[0][k], a[1][k]]) for k in four]
    ay = [jnp.stack([a[2][k], a[3][k]]) for k in four]

    bx = ax[0] + shifted(ax[1], "y", 1) + shifted(ax[2], "y", 2) + shifted(ax[3], "y", 3)
    by = ay[0] + shifted(ay[1], "x", 1) + shifted(ay[2], "x", 2) + shifted(ay[3], "x", 3)

    own = bx[0] + shifted(bx[1], "z", 1) + shifted(by[0], "z", 2) + shifted(by[1], "z", 3)

    norm2 = jnp.broadcast_to(jnp.sum(own * own), (1, LANES))
    for axis in ("x", "y", "z", "pair"):
        norm2 = norm2 + shifted(norm2, axis, 1) + shifted(norm2, axis, 2) + shifted(norm2, axis, 3)
    scale = 1.0 / jnp.maximum(jnp.sqrt(norm2[0, 0] / count), 1.0)

    def from_mate(value):
        near = crossed(value, "pair", 1)
        far = crossed(jnp.where(mask == 3, near, value), "pair", 2)
        return jnp.where(mask == 1, near, far)

    state = jnp.stack([item.reshape(rows, LANES) for item in (master, moment1, moment2)])
    other = from_mate(state)
    theirs = from_mate(own)
    weights = jnp.stack([state[0], other[0]])
    first = jnp.stack([state[1], other[1]])
    second = jnp.stack([state[2], other[2]])
    results = adamw_update(weights, first, second, jnp.stack([own, theirs]), scale)
    return tuple(jnp.where(survive, item, 0.0).reshape(1, 1, 2, shard) for item in results)


def solution(mesh):
    finer = Mesh(mesh.devices.reshape(mesh.shape["pair"], 4, 4, 4), ("pair", "z", "x", "y"))
    dp = ("z", "x", "y")
    in_specs = (P("pair", dp), P("pair", dp), P("pair", dp), P("pair", dp, None), P(dp, None))
    out_specs = (P("pair", dp, None, None), P("pair", dp, None, None), P("pair", dp, None, None))
    return jax.shard_map(on_device, mesh=finer, in_specs=in_specs, out_specs=out_specs, check_vma=False)
```
